8 devices in a mesh: parts: 2 (over z, y), data: 4 (over x, core).
Axes of the slice: x: 2, y: 2, z: 1, core: 2. Of those that a mesh axis runs over, the one named last changes fastest.
Arguments:
- feat_rows: bfloat16 [32768, 3072], P('data')
- labels: int32 [32768], P('data')
- pos_init: float32 [3072, 256], P(None, 'parts'), parts along dimension 1
- mom_init: float32 [3072, 256], P(None, 'parts'), parts along dimension 1
- step_sizes: float32 [16, 256], P(None, 'parts'), parts along dimension 1
Outputs:
- output 1: float32 [3072, 256], P(None, 'parts'), parts along dimension 1
- output 2: float32 [3072, 256], P(None, 'parts'), parts along dimension 1
- output 3: float32 [16, 256], P(None, 'parts'), parts along dimension 1
There are 2 independent parts. The reference program is written for one: setup_inputs(seed, part) draws one part's arguments, and reference() takes and returns one part's arrays. A program takes and returns all parts, laid end to end along the dimension named above; an argument that names none is the same for every part.
All inputs are finite; a program needn't handle non-finite values.
Results may differ from the reference program's by a relative error of at most 0.001.
Values are sent between devices in bfloat16 or wider.
A program may use at most 1 GiB of HBM per device.

```python
import jax
import jax.numpy as jnp
from jax import lax

ROWS_DEV = 8192
GROUP_DEVS = 4
FEATURES = 3072
CHAINS = 128
LEAPFROG = 16

ROWS_TOTAL = ROWS_DEV * GROUP_DEVS
PRIOR_VAR = 4.0
STEP_BASE = (ROWS_DEV + ROWS_TOTAL / FEATURES) ** -0.5
MOM_SCALE = (ROWS_TOTAL / FEATURES) ** 0.5


def setup_inputs(seed: int = 0, part: int = 0) -> dict:
    base_key = jax.random.key(seed)
    key_rate, key_label, key_noise, key_dir, key_strong = jax.random.split(base_key, 5)
    part_key = jax.random.fold_in(jax.random.key(seed + 1), part)
    key_pos, key_mom, key_step = jax.random.split(part_key, 3)
    shard_of_row = jnp.arange(ROWS_TOTAL) // ROWS_DEV
    label_rate = jax.random.randint(key_rate, (GROUP_DEVS,), 1, 16)
    label_draws = jax.random.randint(key_label, (ROWS_TOTAL,), 0, 16)
    labels = (label_draws < label_rate[shard_of_row]).astype(jnp.int32)
    label_sign = (2 * labels - 1).astype(jnp.float32)
    direction = jax.random.normal(key_dir, (FEATURES,), jnp.float32)
    noise_vals = jax.random.normal(key_noise, (ROWS_TOTAL, FEATURES), jnp.float32)
    noise_part = (0.5 / FEATURES ** 0.5) * (noise_vals + label_sign[:, None] * direction[None, :] / FEATURES ** 0.5)
    col_index = jnp.arange(FEATURES)
    strong_mask = ((col_index[None, :] % GROUP_DEVS) == (shard_of_row[:, None] % FEATURES)).astype(jnp.float32)
    strong_count = jnp.sum(strong_mask, axis=1, keepdims=True)
    strong_vals = 1.0 + 0.5 * jax.random.normal(key_strong, (ROWS_TOTAL, FEATURES), jnp.float32)
    feat_rows = (noise_part + strong_mask * strong_vals / jnp.sqrt(strong_count)).astype(jnp.bfloat16)
    pos_init = 0.5 * jax.random.normal(key_pos, (FEATURES, CHAINS), jnp.float32)
    mom_init = (0.5 * MOM_SCALE) * jax.random.normal(key_mom, (FEATURES, CHAINS), jnp.float32)
    step_sizes = STEP_BASE * jax.random.uniform(key_step, (LEAPFROG, CHAINS), jnp.float32, 0.6, 0.9)
    return {"feat_rows": feat_rows, "labels": labels, "pos_init": pos_init, "mom_init": mom_init, "step_sizes": step_sizes}


def potential_terms(feat_rows, labels, positions):
    pos_half = positions.astype(jnp.bfloat16)
    feat_blocks = feat_rows.reshape(GROUP_DEVS, ROWS_DEV, FEATURES)
    label_blocks = labels.astype(jnp.float32).reshape(GROUP_DEVS, ROWS_DEV, 1)

    def block_step(running, block_in):
        grad_acc, loss_acc = running
        block_rows, block_labels = block_in
        logits = jnp.dot(block_rows, pos_half, preferred_element_type=jnp.float32)
        residual = (block_labels - jax.nn.sigmoid(logits)).astype(jnp.bfloat16)
        grad_acc = grad_acc + jnp.dot(block_rows.T, residual, preferred_element_type=jnp.float32)
        loss_acc = loss_acc + jnp.sum(jax.nn.softplus(logits) - block_labels * logits, axis=0)
        return (grad_acc, loss_acc), None

    zero_state = (jnp.zeros((FEATURES, CHAINS), jnp.float32), jnp.zeros((CHAINS,), jnp.float32))
    (grad_lik, loss_lik), _ = lax.scan(block_step, zero_state, (feat_blocks, label_blocks))
    gradient = grad_lik - positions / PRIOR_VAR
    potential = loss_lik + jnp.sum(positions * positions, axis=0) / (2.0 * PRIOR_VAR)
    return gradient, potential


def reference(feat_rows, labels, pos_init, mom_init, step_sizes):
    grad_init, _ = potential_terms(feat_rows, labels, pos_init)

    def leap_step(loop_state, step_size):
        positions, momentum, gradient = loop_state
        momentum = momentum + 0.5 * step_size * gradient
        positions = positions + step_size * momentum
        gradient, potential = potential_terms(feat_rows, labels, positions)
        momentum = momentum + 0.5 * step_size * gradient
        energy = potential + 0.5 * jnp.sum(momentum * momentum, axis=0)
        return (positions, momentum, gradient), energy

    (positions, momentum, _), energies = lax.scan(leap_step, (pos_init, mom_init, grad_init), step_sizes)
    return positions, momentum, energies
```

```python
import functools

import jax
import jax.numpy as jnp
from jax import lax
from jax.experimental import pallas as pl
from jax.experimental.pallas import tpu as pltpu
from jax.sharding import PartitionSpec as P

PRIOR_VAR = 4.0
MESH = pl.DeviceIdType.MESH
F32 = jnp.float32
BF16 = jnp.bfloat16
LANES = 128
OWNERS = 4


def hmc_kernel(
    rows, feats, steps,
    x_hbm, y_ref, pos_hbm, mom_hbm, eps_ref,
    pos_out, mom_out, h_out,
    xv, zacc, rt, th, gbuf, ra, rb, ps, ts, hsum, hall, lacc,
    x_sem, ld_sem,
    a_send, a_recv, b_send, b_recv,
    ts_send, tx_send, ts_recv, tx_recv, tf_send, tf_recv,
    qs_send, qx_send, ql_sem, qs_recv, qx_recv, qf_send, qf_recv,
    ol_sem, hs_send, h_recv,
):
    fb = OWNERS * LANES
    blocks = feats // fb
    zb = 2048
    nb = 1024
    d = lax.axis_index("data")
    sib = d + 1 - 2 * (d % 2)
    par = (d + 2) % 4
    core = d % 2
    xi = d // 2

    def rcopy(src, dst, s_sem, r_sem, dev):
        return pltpu.make_async_remote_copy(
            src_ref=src, dst_ref=dst, send_sem=s_sem, recv_sem=r_sem,
            device_id={"data": dev}, device_id_type=MESH)

    for i in range(rows // nb):
        pltpu.make_async_copy(x_hbm.at[pl.ds(i * nb, nb)], xv.at[pl.ds(i * nb, nb)], x_sem.at[i]).start()
    pos_copy = pltpu.make_async_copy(pos_hbm, gbuf, ld_sem.at[blocks])
    pos_copy.start()
    for j in range(blocks):
        pltpu.make_async_copy(mom_hbm.at[OWNERS * j + d], ps.at[j], ld_sem.at[j]).start()

    barrier = pltpu.get_barrier_semaphore()
    for k in range(1, OWNERS):
        pl.semaphore_signal(barrier, inc=1, device_id={"data": (d + k) % 4}, device_id_type=MESH)
    pl.semaphore_wait(barrier, OWNERS - 1)

    pos_copy.wait()

    def fill_theta(m, _):
        th[pl.ds(pl.multiple_of(m * LANES, LANES), LANES), :] = gbuf[m].astype(BF16)
        return 0

    lax.fori_loop(0, OWNERS * blocks, fill_theta, 0)
    for j in range(blocks):
        ts[j] = gbuf[OWNERS * j + d]
        pltpu.make_async_copy(mom_hbm.at[OWNERS * j + d], ps.at[j], ld_sem.at[j]).wait()
    hsum[...] = jnp.zeros_like(hsum)

    def finish_rows(n0, z):
        zt = z.T
        s = 1.0 - 2.0 * y_ref[:, pl.ds(n0, nb)]
        w = s * zt
        e = jnp.exp(-jnp.abs(w))
        sig = jnp.where(w >= 0.0, 1.0, e) / (1.0 + e)
        rt[:, pl.ds(n0, nb)] = (-s * sig).astype(BF16)
        loss = jnp.maximum(w, 0.0) + jnp.log1p(e)
        acc = loss[:, :LANES]
        for k in range(1, nb // LANES):
            acc = acc + loss[:, k * LANES:(k + 1) * LANES]
        lacc[...] += acc

    def fold_loss(t):
        lt = lacc[...].T
        hsum[t] += jnp.sum(lt.reshape(LANES // 8, 8, LANES), axis=0)
        lacc[...] = jnp.zeros_like(lacc)

    lacc[...] = jnp.zeros_like(lacc)

    def first_rows(i, _):
        n0 = pl.multiple_of(i * nb, nb)
        pltpu.make_async_copy(x_hbm.at[pl.ds(n0, nb)], xv.at[pl.ds(n0, nb)], x_sem.at[i]).wait()
        finish_rows(n0, jnp.dot(xv[pl.ds(n0, nb), :], th[...], preferred_element_type=F32))
        return 0

    lax.fori_loop(0, rows // nb, first_rows, 0)
    fold_loss(0)

    def a_copy(j):
        return rcopy(gbuf.at[pl.ds(OWNERS * j + 2 * (1 - core), 2)], ra.at[pl.ds(2 * j, 2)], a_send.at[j], a_recv.at[j], sib)

    def b_copy(j):
        return rcopy(gbuf.at[OWNERS * j + 2 * core + 1 - xi], rb.at[j], b_send.at[j], b_recv.at[j], par)

    def th_rows(j, owner):
        return th.at[pl.ds(pl.multiple_of((OWNERS * j + owner) * LANES, LANES), LANES)]

    def ts_copy(j):
        return rcopy(th_rows(j, d), th_rows(j, d), ts_send.at[j], ts_recv.at[j], sib)

    def tx_copy(j):
        return rcopy(th_rows(j, d), th_rows(j, d), tx_send.at[j], tx_recv.at[j], par)

    def tf_copy(j):
        return rcopy(th_rows(j, par), th_rows(j, par), tf_send.at[j], tf_recv.at[j], sib)

    def stage1(j):
        a_copy(j).wait()
        away = OWNERS * j + 2 * core + 1 - xi
        gbuf[away] = gbuf[away] + ra[2 * j + 1 - xi]
        b_copy(j).start()

    def gradient(j):
        b_copy(j).wait()
        mine = OWNERS * j + 2 * core + xi
        g = (gbuf[mine] + ra[2 * j + xi] + rb[j]).T
        return g - ts[j] * (1.0 / PRIOR_VAR)

    def half_kick(j, t, g):
        p = ps[j] + (0.5 * eps_ref[pl.ds(t, 1), :]) * g
        q = ts[j]
        e = 0.5 * (p * p) + (0.5 / PRIOR_VAR) * (q * q)
        hsum[t] += jnp.sum(e.reshape(LANES // 8, 8, LANES), axis=0)
        return p, q

    def stage2(j, t):
        g = gradient(j)
        p, q = half_kick(j, t, g)
        step = eps_ref[pl.ds(t + 1, 1), :]
        p = p + (0.5 * step) * g
        q = q + step * p
        ps[j] = p
        ts[j] = q
        th[pl.ds(pl.multiple_of((OWNERS * j + d) * LANES, LANES), LANES), :] = q.astype(BF16)
        tx_copy(j).start()
        ts_copy(j).start()

    def stage3(j):
        tx_copy(j).wait()
        tf_copy(j).start()

    def stage4(j):
        ts_copy(j).wait()
        tf_copy(j).wait()

    def grad_block(j):
        c0 = pl.multiple_of(j * fb, fb)
        res = jnp.dot(rt[...], xv[:, pl.ds(c0, fb)], preferred_element_type=F32)
        for k in range(OWNERS):
            gbuf[OWNERS * j + 2 * (k % 2) + k // 2] = res[:, k * LANES:(k + 1) * LANES]
        a_copy(j).start()

    def logit_block(j):
        def body(i, _):
            n0 = pl.multiple_of(i * zb, zb)
            z = jnp.dot(xv[pl.ds(n0, zb), j * fb:(j + 1) * fb], th[j * fb:(j + 1) * fb, :], preferred_element_type=F32)
            if j == 0:
                zacc[pl.ds(n0, zb), :] = z
            else:
                zacc[pl.ds(n0, zb), :] += z
            return 0

        lax.fori_loop(0, rows // zb, body, 0)

    def last_block(j):
        def body(i, _):
            n0 = pl.multiple_of(i * nb, nb)
            z = jnp.dot(xv[pl.ds(n0, nb), j * fb:(j + 1) * fb], th[j * fb:(j + 1) * fb, :], preferred_element_type=F32)
            finish_rows(n0, zacc[pl.ds(n0, nb), :] + z)
            return 0

        lax.fori_loop(0, rows // nb, body, 0)

    def own_copies(src, out, j, local, s_s, s_r, x_s, x_r):
        row = OWNERS * j + d
        return (
            pltpu.make_async_copy(src.at[j], out.at[row], local.at[j]),
            rcopy(src.at[j], out.at[row], x_s.at[j], x_r.at[j], par),
            rcopy(src.at[j], out.at[row], s_s.at[j], s_r.at[j], sib),
        )

    def pos_copies(j):
        return own_copies(ts, pos_out, j, ql_sem, qs_send, qs_recv, qx_send, qx_recv)

    def mom_copies(j):
        return own_copies(ps, mom_out, j, ol_sem, ts_send, ts_recv, tx_send, tx_recv)

    def pos_forward(j):
        row = OWNERS * j + par
        return rcopy(pos_out.at[row], pos_out.at[row], qf_send.at[j], qf_recv.at[j], sib)

    def mom_forward(j):
        row = OWNERS * j + par
        return rcopy(mom_out.at[row], mom_out.at[row], tf_send.at[j], tf_recv.at[j], sib)

    def leap(t, _):
        def gbody(j, _):
            grad_block(j)

            @pl.when(j >= 1)
            def _():
                stage1(j - 1)

            @pl.when(j >= 4)
            def _():
                stage2(j - 4, t)

            return 0

        lax.fori_loop(0, blocks, gbody, 0)
        stage1(blocks - 1)
        stage2(2, t)
        stage3(0)
        stage2(3, t)
        stage3(1)
        stage4(0)
        logit_block(0)
        stage2(4, t)
        stage2(5, t)

        @pl.when(t == steps - 1)
        def _():
            for j in range(blocks):
                for c in pos_copies(j):
                    c.start()

        stage3(2)
        stage4(1)
        logit_block(1)
        stage3(3)
        stage3(4)
        stage4(2)
        logit_block(2)
        stage3(5)
        stage4(3)
        logit_block(3)
        stage4(4)
        logit_block(4)
        stage4(5)
        last_block(5)
        fold_loss(t + 1)
        return 0

    lax.fori_loop(0, steps, leap, 0)

    for j in range(blocks):
        for c in pos_copies(j)[:2]:
            c.wait()
        pos_forward(j).start()

    def final_stage2(j):
        g = gradient(j)
        p, _ = half_kick(j, steps, g)
        ps[j] = p
        for c in mom_copies(j):
            c.start()

    def final_body(j, _):
        grad_block(j)

        @pl.when(j >= 1)
        def _():
            stage1(j - 1)

        @pl.when(j >= 4)
        def _():
            final_stage2(j - 4)

        return 0

    lax.fori_loop(0, blocks, final_body, 0)
    stage1(blocks - 1)
    for j in range(2, blocks):
        final_stage2(j)

    hall[d] = jnp.sum(hsum[...], axis=1)[1:]
    h_copies = [
        rcopy(hall.at[d], hall.at[d], hs_send.at[k - 1], h_recv.at[k - 1], (d + k) % 4)
        for k in range(1, OWNERS)
    ]
    for c in h_copies:
        c.start()
    for j in range(blocks):
        local, cross, side = mom_copies(j)
        cross.wait()
        mom_forward(j).start()
        local.wait()
        side.wait()
    for c in h_copies:
        c.wait()
    h_out[...] = hall[0] + hall[1] + hall[2] + hall[3]
    for j in range(blocks):
        pos_copies(j)[2].wait()
        pos_forward(j).wait()
        mom_forward(j).wait()


def solution(mesh):
    row_spec = P("data", None)
    chain_spec = P(None, "parts")

    def local_chains(feat_rows, labels, pos_init, mom_init, step_sizes):
        rows, feats = feat_rows.shape
        steps, chains = step_sizes.shape
        tiles = feats // LANES
        blocks = tiles // OWNERS
        label_row = labels.astype(F32)[None, :]
        eps = jnp.concatenate([jnp.zeros((1, chains), F32), step_sizes], axis=0)
        dma = pltpu.SemaphoreType.DMA
        any_space = pl.BlockSpec(memory_space=pl.ANY)
        vmem = pl.BlockSpec(memory_space=pltpu.VMEM)
        cube = jax.ShapeDtypeStruct((tiles, LANES, chains), F32)
        positions, momentum, energies = pl.pallas_call(
            functools.partial(hmc_kernel, rows, feats, steps),
            out_shape=(cube, cube, jax.ShapeDtypeStruct((steps, chains), F32)),
            in_specs=[any_space, vmem, any_space, any_space, vmem],
            out_specs=(any_space, any_space, vmem),
            scratch_shapes=[
                pltpu.VMEM((rows, feats), BF16),
                pltpu.VMEM((rows, chains), F32),
                pltpu.VMEM((chains, rows), BF16),
                pltpu.VMEM((feats, chains), BF16),
                pltpu.VMEM((tiles, LANES, chains), F32),
                pltpu.VMEM((2 * blocks, LANES, chains), F32),
                pltpu.VMEM((blocks, LANES, chains), F32),
                pltpu.VMEM((blocks, LANES, chains), F32),
                pltpu.VMEM((blocks, LANES, chains), F32),
                pltpu.VMEM((steps + 1, 8, chains), F32),
                pltpu.VMEM((OWNERS, steps, chains), F32),
                pltpu.VMEM((chains, LANES), F32),
                dma((rows // 1024,)),
                dma((blocks + 1,)),
            ]
            + [dma((blocks,)) for _ in range(10)]
            + [dma((blocks,)) for _ in range(7)]
            + [dma((blocks,)), dma((OWNERS - 1,)), dma((OWNERS - 1,))],
            compiler_params=pltpu.CompilerParams(
                collective_id=0, has_side_effects=True, vmem_limit_bytes=67043328),
            name="hmc",
        )(feat_rows, label_row, pos_init.reshape(cube.shape), mom_init.reshape(cube.shape), eps)
        return positions.reshape(feats, chains), momentum.reshape(feats, chains), energies

    return jax.shard_map(
        local_chains, mesh=mesh,
        in_specs=(row_spec, P("data"), chain_spec, chain_spec, chain_spec),
        out_specs=(chain_spec, chain_spec, chain_spec), check_vma=False)
```

```python
import functools

import jax
import jax.numpy as jnp
from jax import lax
from jax.experimental import pallas as pl
from jax.experimental.pallas import tpu as pltpu
from jax.sharding import PartitionSpec as P

PRIOR_VAR = 4.0
MESH = pl.DeviceIdType.MESH
F32 = jnp.float32
BF16 = jnp.bfloat16
LANES = 128
OWNERS = 4


def hmc_kernel(
    rows, feats, steps,
    x_hbm, y_ref, pos_hbm, mom_hbm, eps_ref,
    pos_out, mom_out, h_out,
    xv, zs, rt, th, gbuf, ra, rb, ps, ts, hsum, hall, lacc,
    x_sem, ld_sem,
    a_send, a_recv, b_send, b_recv,
    ts_send, tx_send, ts_recv, tx_recv, tf_send, tf_recv,
    qs_send, qx_send, ql_sem, qs_recv, qx_recv, qf_send, qf_recv,
    ol_sem, hs_send, h_recv,
):
    fb = OWNERS * LANES
    blocks = feats // fb
    nb = 1024
    d = lax.axis_index("data")
    sib = d + 1 - 2 * (d % 2)
    par = (d + 2) % 4
    core = d % 2
    xi = d // 2

    def rcopy(src, dst, s_sem, r_sem, dev):
        return pltpu.make_async_remote_copy(
            src_ref=src, dst_ref=dst, send_sem=s_sem, recv_sem=r_sem,
            device_id={"data": dev}, device_id_type=MESH)

    def x_copy(i):
        span = pl.ds(pl.multiple_of(i * nb, nb), nb)
        return pltpu.make_async_copy(x_hbm.at[span], xv.at[span], x_sem.at[i])

    pos_copy = pltpu.make_async_copy(pos_hbm, gbuf, ld_sem.at[blocks])
    pos_copy.start()
    for i in range(rows // nb):
        x_copy(i).start()
    for j in range(blocks):
        pltpu.make_async_copy(mom_hbm.at[OWNERS * j + d], ps.at[j], ld_sem.at[j]).start()

    barrier = pltpu.get_barrier_semaphore()
    for k in range(1, OWNERS):
        pl.semaphore_signal(barrier, inc=1, device_id={"data": (d + k) % 4}, device_id_type=MESH)
    pl.semaphore_wait(barrier, OWNERS - 1)

    pos_copy.wait()

    def fill_theta(m, _):
        th[pl.ds(pl.multiple_of(m * LANES, LANES), LANES), :] = gbuf[m].astype(BF16)
        return 0

    lax.fori_loop(0, OWNERS * blocks, fill_theta, 0)
    for j in range(blocks):
        ts[j] = gbuf[OWNERS * j + d]
        pltpu.make_async_copy(mom_hbm.at[OWNERS * j + d], ps.at[j], ld_sem.at[j]).wait()
    hsum[...] = jnp.zeros_like(hsum)
    lacc[...] = jnp.zeros_like(lacc)

    def residual(n0, width, zt):
        half = y_ref[:, pl.ds(n0, width)]
        rt[:, pl.ds(n0, width)] = (half - 0.5 * jnp.tanh(0.5 * zt)).astype(BF16)

    def loss_rows(i):
        acc = jnp.zeros((LANES, LANES), F32)
        for k in range(nb // LANES):
            n0 = pl.multiple_of(i * nb + k * LANES, LANES)
            zt = zs[pl.ds(n0, LANES), :]
            mag = jnp.abs(zt)
            zs[pl.ds(n0, LANES), :] = jnp.zeros((LANES, LANES), F32)
            acc += 0.5 * mag - y_ref[:, pl.ds(n0, LANES)] * zt + jnp.log1p(jnp.exp(-mag))
        lacc[...] += acc

    def loss_span(lo, hi):
        lax.fori_loop(lo, hi, lambda i, _: (loss_rows(i), 0)[1], 0)

    def fold_loss(t):
        lt = lacc[...].T
        hsum[t] += jnp.sum(lt.reshape(LANES // 8, 8, LANES), axis=0)
        lacc[...] = jnp.zeros_like(lacc)

    def a_copy(j):
        return rcopy(gbuf.at[pl.ds(OWNERS * j + 2 * (1 - core), 2)], ra.at[pl.ds(2 * j, 2)], a_send.at[j], a_recv.at[j], sib)

    def b_copy(j):
        return rcopy(gbuf.at[OWNERS * j + 2 * core + 1 - xi], rb.at[j], b_send.at[j], b_recv.at[j], par)

    def th_rows(j, owner):
        return th.at[pl.ds(pl.multiple_of((OWNERS * j + owner) * LANES, LANES), LANES)]

    def ts_copy(j):
        return rcopy(th_rows(j, d), th_rows(j, d), ts_send.at[j], ts_recv.at[j], sib)

    def tx_copy(j):
        return rcopy(th_rows(j, d), th_rows(j, d), tx_send.at[j], tx_recv.at[j], par)

    def tf_copy(j):
        return rcopy(th_rows(j, par), th_rows(j, par), tf_send.at[j], tf_recv.at[j], sib)

    def own_copies(src, out, j, local, s_s, s_r, x_s, x_r):
        row = OWNERS * j + d
        return (
            lambda: pltpu.make_async_copy(src.at[j], out.at[row], local.at[j]),
            lambda: rcopy(src.at[j], out.at[row], x_s.at[j], x_r.at[j], par),
            lambda: rcopy(src.at[j], out.at[row], s_s.at[j], s_r.at[j], sib),
        )

    def pos_copies(j):
        return own_copies(ts, pos_out, j, ql_sem, qs_send, qs_recv, qx_send, qx_recv)

    def mom_copies(j):
        return own_copies(ps, mom_out, j, ol_sem, ts_send, ts_recv, tx_send, tx_recv)

    def pos_forward(j):
        row = OWNERS * j + par
        return rcopy(pos_out.at[row], pos_out.at[row], qf_send.at[j], qf_recv.at[j], sib)

    def mom_forward(j):
        row = OWNERS * j + par
        return rcopy(mom_out.at[row], mom_out.at[row], tf_send.at[j], tf_recv.at[j], sib)

    def stage1(j):
        a_copy(j).wait()
        away = OWNERS * j + 2 * core + 1 - xi
        gbuf[away] = gbuf[away] + ra[2 * j + 1 - xi]
        b_copy(j).start()

    def stage2(j, t):
        b_copy(j).wait()
        mine = OWNERS * j + 2 * core + xi
        q = ts[j]
        g = (gbuf[mine] + ra[2 * j + xi] + rb[j]).T - q * (1.0 / PRIOR_VAR)
        p = ps[j] + (0.5 * eps_ref[pl.ds(t, 1), :]) * g
        e = 0.5 * (p * p) + (0.5 / PRIOR_VAR) * (q * q)
        hsum[t] += jnp.sum(e.reshape(LANES // 8, 8, LANES), axis=0)

        @pl.when(t < steps)
        def _():
            step = eps_ref[pl.ds(t + 1, 1), :]
            pn = p + (0.5 * step) * g
            qn = q + step * pn
            th[pl.ds(pl.multiple_of((OWNERS * j + d) * LANES, LANES), LANES), :] = qn.astype(BF16)
            tx_copy(j).start()
            ts_copy(j).start()
            ps[j] = pn
            ts[j] = qn

        @pl.when(t == steps)
        def _():
            ps[j] = p
            for c in mom_copies(j):
                c().start()

    def stage3(j):
        tx_copy(j).wait()
        tf_copy(j).start()

    def stage4(j):
        ts_copy(j).wait()
        tf_copy(j).wait()

    def grad_block(j):
        res = jnp.dot(rt[...], xv[:, j * fb:(j + 1) * fb], preferred_element_type=F32)
        for k in range(OWNERS):
            gbuf[OWNERS * j + 2 * (k % 2) + k // 2] = res[:, k * LANES:(k + 1) * LANES]
        a_copy(j).start()

    def grad_phase(t):
        grad_block(0)
        grad_block(1)
        stage1(0)
        grad_block(2)
        stage1(1)
        grad_block(3)
        stage1(2)
        grad_block(4)
        stage2(0, t)
        stage1(3)
        grad_block(5)
        stage2(1, t)
        stage1(4)

    def logit_block(j):
        cols = pl.ds(pl.multiple_of(j * fb, fb), fb)
        zs[...] += jnp.dot(xv[:, cols], th[cols, :], preferred_element_type=F32)

    def tiles_of(n0):
        return pl.ds(pl.multiple_of(n0, nb), nb)

    def finish_rows(i, z):
        for k in range(nb // LANES):
            zt = z[k * LANES:(k + 1) * LANES].T
            n0 = i * nb + k * LANES
            if not isinstance(n0, int):
                n0 = pl.multiple_of(n0, LANES)
            zs[pl.ds(n0, LANES), :] = zt
            residual(n0, LANES, zt)

    def last_block(j):
        for i in range(rows // nb):
            z = jnp.dot(xv[i * nb:(i + 1) * nb, j * fb:(j + 1) * fb], th[j * fb:(j + 1) * fb, :], preferred_element_type=F32)
            finish_rows(i, zs[i * nb:(i + 1) * nb, :] + z)

    def logit_phase(t):
        def body(j, _):
            @pl.when(j == 0)
            def _():
                stage3(0)

            @pl.when(j == 1)
            def _():
                stage2(3, t)
                stage2(4, t)

            @pl.when(j == 2)
            def _():
                stage2(5, t)

                @pl.when(t == steps - 1)
                def _():
                    for k in range(blocks):
                        for c in pos_copies(k):
                            c().start()

            stage3(j + 1)
            stage4(j)
            logit_block(j)
            return 0

        lax.fori_loop(0, blocks - 1, body, 0)
        stage4(blocks - 1)
        last_block(blocks - 1)

    def first_rows(i, _):
        x_copy(i).wait()
        finish_rows(i, jnp.dot(xv[tiles_of(i * nb), :], th[...], preferred_element_type=F32))
        return 0

    lax.fori_loop(0, rows // nb, first_rows, 0)

    def leap(t, _):
        grad_phase(t)
        loss_span(0, 4)
        stage1(5)
        loss_span(4, 8)
        stage2(2, t)
        fold_loss(t)

        @pl.when(t < steps)
        def _():
            logit_phase(t)

        return 0

    lax.fori_loop(0, steps + 1, leap, 0)

    for j in range(3, blocks):
        stage2(j, steps)
    for j in range(blocks):
        for c in pos_copies(j)[:2]:
            c().wait()
        pos_forward(j).start()

    hall[d] = jnp.sum(hsum[...], axis=1)[1:]

    def h_copy(k):
        return rcopy(hall.at[d], hall.at[d], hs_send.at[k - 1], h_recv.at[k - 1], (d + k) % 4)

    for k in range(1, OWNERS):
        h_copy(k).start()
    for j in range(blocks):
        local, cross, side = mom_copies(j)
        cross().wait()
        mom_forward(j).start()
        local().wait()
        side().wait()
    for k in range(1, OWNERS):
        h_copy(k).wait()
    h_out[...] = hall[0] + hall[1] + hall[2] + hall[3]
    for j in range(blocks):
        pos_copies(j)[2]().wait()
        pos_forward(j).wait()
        mom_forward(j).wait()


def solution(mesh):
    row_spec = P("data", None)
    chain_spec = P(None, "parts")

    def local_chains(feat_rows, labels, pos_init, mom_init, step_sizes):
        rows, feats = feat_rows.shape
        steps, chains = step_sizes.shape
        tiles = feats // LANES
        blocks = tiles // OWNERS
        label_row = labels.astype(F32)[None, :] - 0.5
        eps = jnp.concatenate([jnp.zeros((1, chains), F32), step_sizes], axis=0)
        dma = pltpu.SemaphoreType.DMA
        any_space = pl.BlockSpec(memory_space=pl.ANY)
        vmem = pl.BlockSpec(memory_space=pltpu.VMEM)
        cube = jax.ShapeDtypeStruct((tiles, LANES, chains), F32)
        positions, momentum, energies = pl.pallas_call(
            functools.partial(hmc_kernel, rows, feats, steps),
            out_shape=(cube, cube, jax.ShapeDtypeStruct((steps, chains), F32)),
            in_specs=[any_space, vmem, any_space, any_space, vmem],
            out_specs=(any_space, any_space, vmem),
            scratch_shapes=[
                pltpu.VMEM((rows, feats), BF16),
                pltpu.VMEM((rows, chains), F32),
                pltpu.VMEM((chains, rows), BF16),
                pltpu.VMEM((feats, chains), BF16),
                pltpu.VMEM((tiles, LANES, chains), F32),
                pltpu.VMEM((2 * blocks, LANES, chains), F32),
                pltpu.VMEM((blocks, LANES, chains), F32),
                pltpu.VMEM((blocks, LANES, chains), F32),
                pltpu.VMEM((blocks, LANES, chains), F32),
                pltpu.VMEM((steps + 1, 8, chains), F32),
                pltpu.VMEM((OWNERS, steps, chains), F32),
                pltpu.VMEM((chains, LANES), F32),
                dma((rows // 1024,)),
                dma((blocks + 1,)),
            ]
            + [dma((blocks,)) for _ in range(10)]
            + [dma((blocks,)) for _ in range(7)]
            + [dma((blocks,)), dma((OWNERS - 1,)), dma((OWNERS - 1,))],
            compiler_params=pltpu.CompilerParams(
                collective_id=0, has_side_effects=True, vmem_limit_bytes=67043328),
            name="hmc",
        )(feat_rows, label_row, pos_init.reshape(cube.shape), mom_init.reshape(cube.shape), eps)
        return positions.reshape(feats, chains), momentum.reshape(feats, chains), energies

    return jax.shard_map(
        local_chains, mesh=mesh,
        in_specs=(row_spec, P("data"), chain_spec, chain_spec, chain_spec),
        out_specs=(chain_spec, chain_spec, chain_spec), check_vma=False)
```

```python
import functools

import jax
import jax.numpy as jnp
from jax import lax
from jax.experimental import pallas as pl
from jax.experimental.pallas import tpu as pltpu
from jax.sharding import PartitionSpec as P

PRIOR_VAR = 4.0
MESH = pl.DeviceIdType.MESH
F32 = jnp.float32
BF16 = jnp.bfloat16
LANES = 128
OWNERS = 4
TURNED = ((0, 0), (1, 1), (3, 0), (4, 1))
PIECES = ((True, 256), (False, 512)) * 5 + ((True, 256),)


def hmc_kernel(
    rows, feats, steps,
    x_hbm, y_ref, pos_hbm, mom_hbm, eps_ref,
    pos_out, mom_out, h_out, turned,
    xv, zs, rt, th, tt, xt, gbuf, ra, rb, ps, ts, hsum, hall, lacc,
    x_sem, ld_sem, w_sem, c_sem,
    a_send, a_recv, b_send, b_recv,
    ts_send, tx_send, ts_recv, tx_recv, tf_send, tf_recv,
    qs_send, qx_send, ql_sem, qs_recv, qx_recv, qf_send, qf_recv,
    ol_sem, hs_send, h_recv,
):
    fb = OWNERS * LANES
    blocks = feats // fb
    nb = 1024
    d = lax.axis_index("data")
    sib = d + 1 - 2 * (d % 2)
    par = (d + 2) % 4
    core = d % 2
    xi = d // 2

    def rcopy(src, dst, s_sem, r_sem, dev):
        return pltpu.make_async_remote_copy(
            src_ref=src, dst_ref=dst, send_sem=s_sem, recv_sem=r_sem,
            device_id={"data": dev}, device_id_type=MESH)

    def x_copy(i):
        span = pl.ds(pl.multiple_of(i * nb, nb), nb)
        return pltpu.make_async_copy(x_hbm.at[span], xv.at[span], x_sem.at[i])

    pos_copy = pltpu.make_async_copy(pos_hbm, gbuf, ld_sem.at[blocks])
    pos_copy.start()
    for i in range(rows // nb):
        x_copy(i).start()
    for j in range(blocks):
        pltpu.make_async_copy(mom_hbm.at[OWNERS * j + d], ps.at[j], ld_sem.at[j]).start()

    barrier = pltpu.get_barrier_semaphore()
    for k in range(1, OWNERS):
        pl.semaphore_signal(barrier, inc=1, device_id={"data": (d + k) % 4}, device_id_type=MESH)
    pl.semaphore_wait(barrier, OWNERS - 1)

    pos_copy.wait()

    def fill_theta(m, _):
        th[pl.ds(pl.multiple_of(m * LANES, LANES), LANES), :] = gbuf[m].astype(BF16)
        return 0

    lax.fori_loop(0, OWNERS * blocks, fill_theta, 0)
    for j in range(blocks):
        ts[j] = gbuf[OWNERS * j + d]
        pltpu.make_async_copy(mom_hbm.at[OWNERS * j + d], ps.at[j], ld_sem.at[j]).wait()
    hsum[...] = jnp.zeros_like(hsum)
    lacc[...] = jnp.zeros_like(lacc)

    def residual(n0, width, zt):
        half = y_ref[:, pl.ds(n0, width)]
        rt[:, pl.ds(n0, width)] = (half - 0.5 * jnp.tanh(0.5 * zt)).astype(BF16)

    def loss_rows(i):
        acc, prod = None, None
        for k in range(nb // LANES):
            n0 = pl.multiple_of(i * nb + k * LANES, LANES)
            zt = zs[pl.ds(n0, LANES), :]
            zs[pl.ds(n0, LANES), :] = jnp.zeros((LANES, LANES), F32)
            mag = jnp.abs(zt)
            line = 0.5 * mag - y_ref[:, pl.ds(n0, LANES)] * zt
            soft = 1.0 + jnp.exp(-mag)
            acc, prod = (line, soft) if acc is None else (acc + line, prod * soft)
        lacc[...] += acc + jnp.log(prod)

    def loss_span(lo, hi):
        lax.fori_loop(lo, hi, lambda i, _: (loss_rows(i), 0)[1], 0)

    def fold_loss(t):
        lt = lacc[...].T
        hsum[t] += jnp.sum(lt.reshape(LANES // 8, 8, LANES), axis=0)
        lacc[...] = jnp.zeros_like(lacc)

    def a_copy(j):
        return rcopy(gbuf.at[pl.ds(OWNERS * j + 2 * (1 - core), 2)], ra.at[pl.ds(2 * j, 2)], a_send.at[j], a_recv.at[j], sib)

    def b_copy(j):
        return rcopy(gbuf.at[OWNERS * j + 2 * core + 1 - xi], rb.at[j], b_send.at[j], b_recv.at[j], par)

    def th_rows(j, owner):
        return th.at[pl.ds(pl.multiple_of((OWNERS * j + owner) * LANES, LANES), LANES)]

    def ts_copy(j):
        return rcopy(th_rows(j, d), th_rows(j, d), ts_send.at[j], ts_recv.at[j], sib)

    def tx_copy(j):
        return rcopy(th_rows(j, d), th_rows(j, d), tx_send.at[j], tx_recv.at[j], par)

    def tf_copy(j):
        return rcopy(th_rows(j, par), th_rows(j, par), tf_send.at[j], tf_recv.at[j], sib)

    def own_copies(src, out, j, local, s_s, s_r, x_s, x_r):
        row = OWNERS * j + d
        return (
            lambda: pltpu.make_async_copy(src.at[j], out.at[row], local.at[j]),
            lambda: rcopy(src.at[j], out.at[row], x_s.at[j], x_r.at[j], par),
            lambda: rcopy(src.at[j], out.at[row], s_s.at[j], s_r.at[j], sib),
        )

    def pos_copies(j):
        return own_copies(ts, pos_out, j, ql_sem, qs_send, qs_recv, qx_send, qx_recv)

    def mom_copies(j):
        return own_copies(ps, mom_out, j, ol_sem, ts_send, ts_recv, tx_send, tx_recv)

    def pos_forward(j):
        row = OWNERS * j + par
        return rcopy(pos_out.at[row], pos_out.at[row], qf_send.at[j], qf_recv.at[j], sib)

    def mom_forward(j):
        row = OWNERS * j + par
        return rcopy(mom_out.at[row], mom_out.at[row], tf_send.at[j], tf_recv.at[j], sib)

    def stage1(j):
        a_copy(j).wait()
        away = OWNERS * j + 2 * core + 1 - xi
        gbuf[away] = gbuf[away] + ra[2 * j + 1 - xi]
        b_copy(j).start()

    def stage2(j, t):
        b_copy(j).wait()
        mine = OWNERS * j + 2 * core + xi
        q = ts[j]
        g = (gbuf[mine] + ra[2 * j + xi] + rb[j]).T - q * (1.0 / PRIOR_VAR)
        p = ps[j] + (0.5 * eps_ref[pl.ds(t, 1), :]) * g
        e = 0.5 * (p * p) + (0.5 / PRIOR_VAR) * (q * q)
        hsum[t] += jnp.sum(e.reshape(LANES // 8, 8, LANES), axis=0)

        @pl.when(t < steps)
        def _():
            step = eps_ref[pl.ds(t + 1, 1), :]
            pn = p + (0.5 * step) * g
            qn = q + step * pn
            th[pl.ds(pl.multiple_of((OWNERS * j + d) * LANES, LANES), LANES), :] = qn.astype(BF16)
            tx_copy(j).start()
            ts_copy(j).start()
            ps[j] = pn
            ts[j] = qn

        @pl.when(t == steps)
        def _():
            ps[j] = p
            for c in mom_copies(j):
                c().start()

    def stage3(j):
        tx_copy(j).wait()
        tf_copy(j).start()

    def stage4(j):
        ts_copy(j).wait()
        tf_copy(j).wait()

    def grad_block(j):
        res = jnp.dot(rt[...], xv[:, j * fb:(j + 1) * fb], preferred_element_type=F32)
        for k in range(OWNERS):
            gbuf[OWNERS * j + 2 * (k % 2) + k // 2] = res[:, k * LANES:(k + 1) * LANES]
        a_copy(j).start()

    def grad_phase(t):
        grad_block(0)
        grad_block(1)
        stage1(0)
        grad_block(2)
        stage1(1)
        grad_block(3)
        stage1(2)
        grad_block(4)
        stage2(0, t)
        stage1(3)
        grad_block(5)
        stage2(1, t)
        stage1(4)

    def logit_pieces(c0, h):
        cols = pl.ds(c0, fb)
        if h == 0:
            tt[...] = th[cols, :].T
        n0 = h * (rows // 2)
        for flat, size in PIECES:
            x = xv[n0:n0 + size, cols]
            if flat:
                yield n0, size, flat, jnp.dot(x, th[cols, :], preferred_element_type=F32)
            else:
                yield n0, size, flat, lax.dot_general(tt[...], x, (((1,), (1,)), ((), ())), preferred_element_type=F32)
            n0 += size

    def chunk_load(k):
        return pltpu.make_async_copy(turned.at[k], xt, c_sem)

    def turned_block(j, k):
        h = TURNED[k][1]
        if h == 0:
            tt[...] = th[pl.ds(pl.multiple_of(j * fb, fb), fb), :].T
        chunk_load(k).wait()
        flats = []
        for flat, size in PIECES:
            flats += [flat] * (size // LANES)
        for i in range(rows // 2 // nb):
            z = jnp.dot(tt[...], xt[i], preferred_element_type=F32)
            for m in range(nb // LANES):
                n0 = i * nb + m * LANES
                tile = slice(h * (rows // 2) + n0, h * (rows // 2) + n0 + LANES)
                zt = z[:, m * LANES:(m + 1) * LANES]
                zs[tile, :] += zt.T if flats[n0 // LANES] else zt
        chunk_load((k + 1) % len(TURNED)).start()

    def make_turned():
        def write(k, i):
            return pltpu.make_async_copy(xt.at[i], turned.at[k, i], w_sem.at[i])

        order = list(range(len(TURNED)))[::-1]
        for k in order:
            j, h = TURNED[k]
            for i in range(rows // 2 // nb):
                if k != order[0]:
                    write(k + 1, i).wait()
                n0 = h * (rows // 2) + i * nb
                xt[i] = xv[n0:n0 + nb, j * fb:(j + 1) * fb].T
                write(k, i).start()
        for i in range(rows // 2 // nb):
            write(0, i).wait()
        chunk_load(0).start()

    def plain_block(j, h):
        for n0, size, flat, z in logit_pieces(pl.multiple_of(j * fb, fb), h):
            if flat:
                zs[n0:n0 + size, :] += z
            else:
                for k in range(0, size, LANES):
                    zs[n0 + k:n0 + k + LANES, :] += z[:, k:k + LANES]

    def logit_block(j, h):
        mine = [k for k in range(len(TURNED)) if TURNED[k][1] == h]
        hit = j == TURNED[mine[0]][0]
        for k in mine[1:]:
            hit = jnp.logical_or(hit, j == TURNED[k][0])
        for k in mine:
            pl.when(j == TURNED[k][0])(functools.partial(turned_block, j, k))
        pl.when(jnp.logical_not(hit))(functools.partial(plain_block, j, h))

    def tiles_of(n0):
        return pl.ds(pl.multiple_of(n0, nb), nb)

    def finish_rows(i, z):
        for k in range(nb // LANES):
            zt = z[k * LANES:(k + 1) * LANES].T
            n0 = i * nb + k * LANES
            if not isinstance(n0, int):
                n0 = pl.multiple_of(n0, LANES)
            zs[pl.ds(n0, LANES), :] = zt
            residual(n0, LANES, zt)

    def last_block(j, h):
        for n0, size, flat, z in logit_pieces(j * fb, h):
            for k in range(0, size, LANES):
                tile = slice(n0 + k, n0 + k + LANES)
                zt = (zs[tile, :] + z[k:k + LANES]).T if flat else zs[tile, :] + z[:, k:k + LANES]
                zs[tile, :] = zt
                residual(n0 + k, LANES, zt)

    def logit_phase(t):
        stage3(0)

        def body(j, _):
            @pl.when(j == 1)
            def _():
                stage2(3, t)

            @pl.when((j == 3) & (t == steps - 1))
            def _():
                for k in range(blocks):
                    for c in pos_copies(k):
                        c().start()

            stage4(j)
            logit_block(j, 0)

            @pl.when(j == 1)
            def _():
                stage2(4, t)

            @pl.when(j == 2)
            def _():
                stage2(5, t)

            stage3(j + 1)
            logit_block(j, 1)
            return 0

        lax.fori_loop(0, blocks - 1, body, 0)
        stage4(blocks - 1)
        last_block(blocks - 1, 0)
        last_block(blocks - 1, 1)

    def first_rows(i, _):
        x_copy(i).wait()
        finish_rows(i, jnp.dot(xv[tiles_of(i * nb), :], th[...], preferred_element_type=F32))
        return 0

    lax.fori_loop(0, rows // nb, first_rows, 0)
    make_turned()

    def leap(t, _):
        grad_phase(t)
        loss_span(0, 4)
        stage1(5)
        loss_span(4, 8)
        stage2(2, t)
        fold_loss(t)

        @pl.when(t < steps)
        def _():
            logit_phase(t)

        return 0

    lax.fori_loop(0, steps + 1, leap, 0)

    chunk_load(0).wait()

    for j in range(3, blocks):
        stage2(j, steps)
    for j in range(blocks):
        for c in pos_copies(j)[:2]:
            c().wait()
        pos_forward(j).start()

    hall[d] = jnp.sum(hsum[...], axis=1)[1:]

    def h_copy(k):
        return rcopy(hall.at[d], hall.at[d], hs_send.at[k - 1], h_recv.at[k - 1], (d + k) % 4)

    for k in range(1, OWNERS):
        h_copy(k).start()
    for j in range(blocks):
        local, cross, side = mom_copies(j)
        cross().wait()
        mom_forward(j).start()
        local().wait()
        side().wait()
    for k in range(1, OWNERS):
        h_copy(k).wait()
    h_out[...] = hall[0] + hall[1] + hall[2] + hall[3]
    for j in range(blocks):
        pos_copies(j)[2]().wait()
        pos_forward(j).wait()
        mom_forward(j).wait()


def solution(mesh):
    row_spec = P("data", None)
    chain_spec = P(None, "parts")

    def local_chains(feat_rows, labels, pos_init, mom_init, step_sizes):
        rows, feats = feat_rows.shape
        steps, chains = step_sizes.shape
        tiles = feats // LANES
        blocks = tiles // OWNERS
        label_row = labels.astype(F32)[None, :] - 0.5
        eps = jnp.concatenate([jnp.zeros((1, chains), F32), step_sizes], axis=0)
        dma = pltpu.SemaphoreType.DMA
        turned_shape = (rows // 2048, OWNERS * LANES, 1024)
        any_space = pl.BlockSpec(memory_space=pl.ANY)
        vmem = pl.BlockSpec(memory_space=pltpu.VMEM)
        cube = jax.ShapeDtypeStruct((tiles, LANES, chains), F32)
        positions, momentum, energies, _ = pl.pallas_call(
            functools.partial(hmc_kernel, rows, feats, steps),
            out_shape=(
                cube, cube, jax.ShapeDtypeStruct((steps, chains), F32),
                jax.ShapeDtypeStruct((len(TURNED),) + turned_shape, BF16)),
            in_specs=[any_space, vmem, any_space, any_space, vmem],
            out_specs=(any_space, any_space, vmem, any_space),
            scratch_shapes=[
                pltpu.VMEM((rows, feats), BF16),
                pltpu.VMEM((rows, chains), F32),
                pltpu.VMEM((chains, rows), BF16),
                pltpu.VMEM((feats, chains), BF16),
                pltpu.VMEM((chains, OWNERS * LANES), BF16),
                pltpu.VMEM(turned_shape, BF16),
                pltpu.VMEM((tiles, LANES, chains), F32),
                pltpu.VMEM((2 * blocks, LANES, chains), F32),
                pltpu.VMEM((blocks, LANES, chains), F32),
                pltpu.VMEM((blocks, LANES, chains), F32),
                pltpu.VMEM((blocks, LANES, chains), F32),
                pltpu.VMEM((steps + 1, 8, chains), F32),
                pltpu.VMEM((OWNERS, steps, chains), F32),
                pltpu.VMEM((chains, LANES), F32),
                dma((rows // 1024,)),
                dma((blocks + 1,)),
                dma((rows // 2048,)),
                dma,
            ]
            + [dma((blocks,)) for _ in range(10)]
            + [dma((blocks,)) for _ in range(7)]
            + [dma((blocks,)), dma((OWNERS - 1,)), dma((OWNERS - 1,))],
            compiler_params=pltpu.CompilerParams(
                collective_id=0, has_side_effects=True, vmem_limit_bytes=67043328),
            name="hmc",
        )(feat_rows, label_row, pos_init.reshape(cube.shape), mom_init.reshape(cube.shape), eps)
        return positions.reshape(feats, chains), momentum.reshape(feats, chains), energies

    return jax.shard_map(
        local_chains, mesh=mesh,
        in_specs=(row_spec, P("data"), chain_spec, chain_spec, chain_spec),
        out_specs=(chain_spec, chain_spec, chain_spec), check_vma=False)
```

```python
import functools

import jax
import jax.numpy as jnp
from jax import lax
from jax.experimental import pallas as pl
from jax.experimental.pallas import tpu as pltpu
from jax.sharding import PartitionSpec as P

PRIOR_VAR = 4.0
MESH = pl.DeviceIdType.MESH
F32 = jnp.float32
BF16 = jnp.bfloat16
LANES = 128
OWNERS = 4
TURNED = ((0, 0), (1, 1), (3, 0), (4, 1))
PIECES = ((True, 256), (False, 512)) * 5 + ((True, 256),)


def hmc_kernel(
    rows, feats, steps,
    x_hbm, y_ref, pos_hbm, mom_hbm, eps_ref,
    pos_out, mom_out, h_out, turned,
    xv, zs, rt, th, tt, xt, gbuf, ra, rb, ps, ts, hsum, hall, lacc,
    x_sem, ld_sem, w_sem, c_sem,
    a_send, a_recv, b_send, b_recv,
    ts_send, tx_send, ts_recv, tx_recv, tf_send, tf_recv,
    qs_send, qx_send, ql_sem, qs_recv, qx_recv, qf_send, qf_recv,
    ol_sem, hs_send, h_recv,
):
    fb = OWNERS * LANES
    blocks = feats // fb
    nb = 1024
    d = lax.axis_index("data")
    sib = d + 1 - 2 * (d % 2)
    par = (d + 2) % 4
    core = d % 2
    xi = d // 2

    def rcopy(src, dst, s_sem, r_sem, dev):
        return pltpu.make_async_remote_copy(
            src_ref=src, dst_ref=dst, send_sem=s_sem, recv_sem=r_sem,
            device_id={"data": dev}, device_id_type=MESH)

    def x_copy(i):
        span = pl.ds(pl.multiple_of(i * nb, nb), nb)
        return pltpu.make_async_copy(x_hbm.at[span], xv.at[span], x_sem.at[i])

    pos_copy = pltpu.make_async_copy(pos_hbm, gbuf, ld_sem.at[blocks])
    pos_copy.start()
    for i in range(rows // nb):
        x_copy(i).start()
    for j in range(blocks):
        pltpu.make_async_copy(mom_hbm.at[OWNERS * j + d], ps.at[j], ld_sem.at[j]).start()

    barrier = pltpu.get_barrier_semaphore()
    for k in range(1, OWNERS):
        pl.semaphore_signal(barrier, inc=1, device_id={"data": (d + k) % 4}, device_id_type=MESH)
    pl.semaphore_wait(barrier, OWNERS - 1)

    pos_copy.wait()

    def fill_theta(m, _):
        th[pl.ds(pl.multiple_of(m * LANES, LANES), LANES), :] = gbuf[m].astype(BF16)
        return 0

    lax.fori_loop(0, OWNERS * blocks, fill_theta, 0)
    for j in range(blocks):
        ts[j] = gbuf[OWNERS * j + d]
        pltpu.make_async_copy(mom_hbm.at[OWNERS * j + d], ps.at[j], ld_sem.at[j]).wait()
    hsum[...] = jnp.zeros_like(hsum)
    lacc[...] = jnp.zeros_like(lacc)

    def residual(n0, width, zt):
        half = y_ref[:, pl.ds(n0, width)]
        rt[:, pl.ds(n0, width)] = (half - 0.5 * jnp.tanh(0.5 * zt)).astype(BF16)

    def loss_rows(i):
        acc, prod = None, None
        for k in range(nb // LANES):
            n0 = pl.multiple_of(i * nb + k * LANES, LANES)
            zt = zs[pl.ds(n0, LANES), :]
            zs[pl.ds(n0, LANES), :] = jnp.zeros((LANES, LANES), F32)
            mag = jnp.abs(zt)
            line = 0.5 * mag - y_ref[:, pl.ds(n0, LANES)] * zt
            soft = 1.0 + jnp.exp(-mag)
            acc, prod = (line, soft) if acc is None else (acc + line, prod * soft)
        lacc[...] += acc + jnp.log(prod)

    def loss_span(lo, hi):
        lax.fori_loop(lo, hi, lambda i, _: (loss_rows(i), 0)[1], 0)

    def fold_loss(t):
        lt = lacc[...].T
        hsum[t] += jnp.sum(lt.reshape(LANES // 8, 8, LANES), axis=0)
        lacc[...] = jnp.zeros_like(lacc)

    def a_copy(j):
        return rcopy(gbuf.at[pl.ds(OWNERS * j + 2 * (1 - core), 2)], ra.at[pl.ds(2 * j, 2)], a_send.at[j], a_recv.at[j], sib)

    def b_copy(j):
        return rcopy(gbuf.at[OWNERS * j + 2 * core + 1 - xi], rb.at[j], b_send.at[j], b_recv.at[j], par)

    def th_rows(j, owner):
        return th.at[pl.ds(pl.multiple_of((OWNERS * j + owner) * LANES, LANES), LANES)]

    def ts_copy(j):
        return rcopy(th_rows(j, d), th_rows(j, d), ts_send.at[j], ts_recv.at[j], sib)

    def tx_copy(j):
        return rcopy(th_rows(j, d), th_rows(j, d), tx_send.at[j], tx_recv.at[j], par)

    def tf_copy(j):
        return rcopy(th_rows(j, par), th_rows(j, par), tf_send.at[j], tf_recv.at[j], sib)

    def own_copies(src, out, j, local, s_s, s_r, x_s, x_r):
        row = OWNERS * j + d
        return (
            lambda: pltpu.make_async_copy(src.at[j], out.at[row], local.at[j]),
            lambda: rcopy(src.at[j], out.at[row], x_s.at[j], x_r.at[j], par),
            lambda: rcopy(src.at[j], out.at[row], s_s.at[j], s_r.at[j], sib),
        )

    def pos_copies(j):
        return own_copies(ts, pos_out, j, ql_sem, qs_send, qs_recv, qx_send, qx_recv)

    def mom_copies(j):
        return own_copies(ps, mom_out, j, ol_sem, ts_send, ts_recv, tx_send, tx_recv)

    def pos_forward(j):
        row = OWNERS * j + par
        return rcopy(pos_out.at[row], pos_out.at[row], qf_send.at[j], qf_recv.at[j], sib)

    def mom_forward(j):
        row = OWNERS * j + par
        return rcopy(mom_out.at[row], mom_out.at[row], tf_send.at[j], tf_recv.at[j], sib)

    def stage1(j):
        a_copy(j).wait()
        away = OWNERS * j + 2 * core + 1 - xi
        gbuf[away] = gbuf[away] + ra[2 * j + 1 - xi]
        b_copy(j).start()

    def stage2(j, t):
        b_copy(j).wait()
        mine = OWNERS * j + 2 * core + xi
        q = ts[j]
        g = (gbuf[mine] + ra[2 * j + xi] + rb[j]).T - q * (1.0 / PRIOR_VAR)
        p = ps[j] + (0.5 * eps_ref[pl.ds(t, 1), :]) * g
        e = 0.5 * (p * p) + (0.5 / PRIOR_VAR) * (q * q)
        hsum[t] += jnp.sum(e.reshape(LANES // 8, 8, LANES), axis=0)

        @pl.when(t < steps)
        def _():
            step = eps_ref[pl.ds(t + 1, 1), :]
            pn = p + (0.5 * step) * g
            qn = q + step * pn
            th[pl.ds(pl.multiple_of((OWNERS * j + d) * LANES, LANES), LANES), :] = qn.astype(BF16)
            tx_copy(j).start()
            ts_copy(j).start()
            ps[j] = pn
            ts[j] = qn

        @pl.when(t == steps)
        def _():
            ps[j] = p
            for c in mom_copies(j):
                c().start()

    def stage3(j):
        tx_copy(j).wait()
        tf_copy(j).start()

    def stage4(j):
        ts_copy(j).wait()
        tf_copy(j).wait()

    def grad_block(j):
        res = jnp.dot(rt[...], xv[:, j * fb:(j + 1) * fb], preferred_element_type=F32)
        for k in range(OWNERS):
            gbuf[OWNERS * j + 2 * (k % 2) + k // 2] = res[:, k * LANES:(k + 1) * LANES]
        a_copy(j).start()

    def grad_phase(t):
        grad_block(0)
        grad_block(1)
        stage1(0)
        grad_block(2)
        stage1(1)
        grad_block(3)
        stage1(2)
        grad_block(4)
        stage2(0, t)
        stage1(3)
        grad_block(5)
        stage2(1, t)
        stage1(4)

    def logit_pieces(c0, h):
        cols = pl.ds(c0, fb)
        if h == 0:
            tt[...] = th[cols, :].T
        n0 = h * (rows // 2)
        for flat, size in PIECES:
            x = xv[n0:n0 + size, cols]
            if flat:
                yield n0, size, flat, jnp.dot(x, th[cols, :], preferred_element_type=F32)
            else:
                yield n0, size, flat, lax.dot_general(tt[...], x, (((1,), (1,)), ((), ())), preferred_element_type=F32)
            n0 += size

    def chunk_load(k):
        return pltpu.make_async_copy(turned.at[k], xt, c_sem)

    def turned_block(j, k):
        h = TURNED[k][1]
        if h == 0:
            tt[...] = th[pl.ds(pl.multiple_of(j * fb, fb), fb), :].T
        chunk_load(k).wait()
        flats = []
        for flat, size in PIECES:
            flats += [flat] * (size // LANES)
        for i in range(rows // 2 // nb):
            z = jnp.dot(tt[...], xt[i], preferred_element_type=F32)
            for m in range(nb // LANES):
                n0 = i * nb + m * LANES
                tile = slice(h * (rows // 2) + n0, h * (rows // 2) + n0 + LANES)
                zt = z[:, m * LANES:(m + 1) * LANES]
                zs[tile, :] += zt.T if flats[n0 // LANES] else zt
        chunk_load((k + 1) % len(TURNED)).start()

    def turned_write(i, m):
        half = rows // 2 // nb
        slot = 2 * (i % 2) + m
        return pltpu.make_async_copy(xt.at[slot], turned.at[2 * m + i // half, i % half], w_sem.at[slot])

    def make_turned(i):
        for m in range(2):
            pl.when(i >= 2)(lambda m=m: turned_write(i - 2, m).wait())
            c0 = pl.multiple_of((3 * m + i // (rows // 2 // nb)) * fb, fb)
            xt[2 * (i % 2) + m] = xv[tiles_of(i * nb), pl.ds(c0, fb)].T
        for m in range(2):
            turned_write(i, m).start()

    def plain_block(j, h):
        for n0, size, flat, z in logit_pieces(pl.multiple_of(j * fb, fb), h):
            if flat:
                zs[n0:n0 + size, :] += z
            else:
                for k in range(0, size, LANES):
                    zs[n0 + k:n0 + k + LANES, :] += z[:, k:k + LANES]

    def logit_block(j, h):
        mine = [k for k in range(len(TURNED)) if TURNED[k][1] == h]
        hit = j == TURNED[mine[0]][0]
        for k in mine[1:]:
            hit = jnp.logical_or(hit, j == TURNED[k][0])
        for k in mine:
            pl.when(j == TURNED[k][0])(functools.partial(turned_block, j, k))
        pl.when(jnp.logical_not(hit))(functools.partial(plain_block, j, h))

    def tiles_of(n0):
        return pl.ds(pl.multiple_of(n0, nb), nb)

    def finish_rows(i, z):
        for k in range(nb // LANES):
            zt = z[k * LANES:(k + 1) * LANES].T
            n0 = i * nb + k * LANES
            if not isinstance(n0, int):
                n0 = pl.multiple_of(n0, LANES)
            zs[pl.ds(n0, LANES), :] = zt
            residual(n0, LANES, zt)

    def last_block(j, h):
        for n0, size, flat, z in logit_pieces(j * fb, h):
            for k in range(0, size, LANES):
                tile = slice(n0 + k, n0 + k + LANES)
                zt = (zs[tile, :] + z[k:k + LANES]).T if flat else zs[tile, :] + z[:, k:k + LANES]
                zs[tile, :] = zt
                residual(n0 + k, LANES, zt)

    def logit_phase(t):
        stage3(0)

        def body(j, _):
            @pl.when(j == 1)
            def _():
                stage2(3, t)

            @pl.when((j == 3) & (t == steps - 1))
            def _():
                for k in range(blocks):
                    for c in pos_copies(k):
                        c().start()

            stage4(j)
            logit_block(j, 0)

            @pl.when(j == 1)
            def _():
                stage2(4, t)

            @pl.when(j == 2)
            def _():
                stage2(5, t)

            stage3(j + 1)
            logit_block(j, 1)
            return 0

        lax.fori_loop(0, blocks - 1, body, 0)
        stage4(blocks - 1)
        last_block(blocks - 1, 0)
        last_block(blocks - 1, 1)

    def first_rows(i, _):
        x_copy(i).wait()
        make_turned(i)
        finish_rows(i, jnp.dot(xv[tiles_of(i * nb), :], th[...], preferred_element_type=F32))
        return 0

    lax.fori_loop(0, rows // nb, first_rows, 0)
    for i in range(rows // nb - 2, rows // nb):
        for m in range(2):
            turned_write(i, m).wait()
    chunk_load(0).start()

    def leap(t, _):
        grad_phase(t)
        loss_span(0, 4)
        stage2(2, t)
        stage1(5)
        loss_span(4, 8)
        fold_loss(t)

        @pl.when(t < steps)
        def _():
            logit_phase(t)

        return 0

    lax.fori_loop(0, steps + 1, leap, 0)

    chunk_load(0).wait()

    for j in range(3, blocks):
        stage2(j, steps)
    for j in range(blocks):
        for c in pos_copies(j)[:2]:
            c().wait()
        pos_forward(j).start()

    hall[d] = jnp.sum(hsum[...], axis=1)[1:]

    def h_copy(k):
        return rcopy(hall.at[d], hall.at[d], hs_send.at[k - 1], h_recv.at[k - 1], (d + k) % 4)

    for k in range(1, OWNERS):
        h_copy(k).start()
    for j in range(blocks):
        local, cross, side = mom_copies(j)
        cross().wait()
        mom_forward(j).start()
        local().wait()
        side().wait()
    for k in range(1, OWNERS):
        h_copy(k).wait()
    h_out[...] = hall[0] + hall[1] + hall[2] + hall[3]
    for j in range(blocks):
        pos_copies(j)[2]().wait()
        pos_forward(j).wait()
        mom_forward(j).wait()


def solution(mesh):
    row_spec = P("data", None)
    chain_spec = P(None, "parts")

    def local_chains(feat_rows, labels, pos_init, mom_init, step_sizes):
        rows, feats = feat_rows.shape
        steps, chains = step_sizes.shape
        tiles = feats // LANES
        blocks = tiles // OWNERS
        label_row = labels.astype(F32)[None, :] - 0.5
        eps = jnp.concatenate([jnp.zeros((1, chains), F32), step_sizes], axis=0)
        dma = pltpu.SemaphoreType.DMA
        turned_shape = (rows // 2048, OWNERS * LANES, 1024)
        any_space = pl.BlockSpec(memory_space=pl.ANY)
        vmem = pl.BlockSpec(memory_space=pltpu.VMEM)
        cube = jax.ShapeDtypeStruct((tiles, LANES, chains), F32)
        positions, momentum, energies, _ = pl.pallas_call(
            functools.partial(hmc_kernel, rows, feats, steps),
            out_shape=(
                cube, cube, jax.ShapeDtypeStruct((steps, chains), F32),
                jax.ShapeDtypeStruct((len(TURNED),) + turned_shape, BF16)),
            in_specs=[any_space, vmem, any_space, any_space, vmem],
            out_specs=(any_space, any_space, vmem, any_space),
            scratch_shapes=[
                pltpu.VMEM((rows, feats), BF16),
                pltpu.VMEM((rows, chains), F32),
                pltpu.VMEM((chains, rows), BF16),
                pltpu.VMEM((feats, chains), BF16),
                pltpu.VMEM((chains, OWNERS * LANES), BF16),
                pltpu.VMEM(turned_shape, BF16),
                pltpu.VMEM((tiles, LANES, chains), F32),
                pltpu.VMEM((2 * blocks, LANES, chains), F32),
                pltpu.VMEM((blocks, LANES, chains), F32),
                pltpu.VMEM((blocks, LANES, chains), F32),
                pltpu.VMEM((blocks, LANES, chains), F32),
                pltpu.VMEM((steps + 1, 8, chains), F32),
                pltpu.VMEM((OWNERS, steps, chains), F32),
                pltpu.VMEM((chains, LANES), F32),
                dma((rows // 1024,)),
                dma((blocks + 1,)),
                dma((rows // 2048,)),
                dma,
            ]
            + [dma((blocks,)) for _ in range(10)]
            + [dma((blocks,)) for _ in range(7)]
            + [dma((blocks,)), dma((OWNERS - 1,)), dma((OWNERS - 1,))],
            compiler_params=pltpu.CompilerParams(
                collective_id=0, has_side_effects=True, vmem_limit_bytes=67043328),
            name="hmc",
        )(feat_rows, label_row, pos_init.reshape(cube.shape), mom_init.reshape(cube.shape), eps)
        return positions.reshape(feats, chains), momentum.reshape(feats, chains), energies

    return jax.shard_map(
        local_chains, mesh=mesh,
        in_specs=(row_spec, P("data"), chain_spec, chain_spec, chain_spec),
        out_specs=(chain_spec, chain_spec, chain_spec), check_vma=False)
```

```python
import functools

import jax
import jax.numpy as jnp
from jax import lax
from jax.experimental import pallas as pl
from jax.experimental.pallas import tpu as pltpu
from jax.sharding import PartitionSpec as P

PRIOR_VAR = 4.0
MESH = pl.DeviceIdType.MESH
F32 = jnp.float32
BF16 = jnp.bfloat16
LANES = 128
OWNERS = 4
TURNED = ((0, 0), (1, 1), (3, 0), (4, 1))
PIECES = ((True, 256), (False, 512)) * 5 + ((True, 256),)


def hmc_kernel(
    rows, feats, steps,
    x_hbm, y_ref, pos_hbm, mom_hbm, eps_ref,
    pos_out, mom_out, h_out, turned,
    xv, zs, rt, th, tt, xt, gbuf, ra, rb, ps, ts, hsum, hall, lacc,
    x_sem, ld_sem, w_sem, c_sem,
    a_send, a_recv, b_send, b_recv,
    ts_send, tx_send, ts_recv, tx_recv, tf_send, tf_recv,
    qs_send, qx_send, ql_sem, qs_recv, qx_recv, qf_send, qf_recv,
    ol_sem, hs_send, h_recv,
):
    fb = OWNERS * LANES
    blocks = feats // fb
    nb = 1024
    d = lax.axis_index("data")
    sib = d + 1 - 2 * (d % 2)
    par = (d + 2) % 4
    core = d % 2
    xi = d // 2

    def rcopy(src, dst, s_sem, r_sem, dev):
        return pltpu.make_async_remote_copy(
            src_ref=src, dst_ref=dst, send_sem=s_sem, recv_sem=r_sem,
            device_id={"data": dev}, device_id_type=MESH)

    def x_copy(i):
        span = pl.ds(pl.multiple_of(i * nb, nb), nb)
        return pltpu.make_async_copy(x_hbm.at[span], xv.at[span], x_sem.at[i])

    pos_copy = pltpu.make_async_copy(pos_hbm, gbuf, ld_sem.at[blocks])
    pos_copy.start()
    for i in range(rows // nb):
        x_copy(i).start()
    for j in range(blocks):
        pltpu.make_async_copy(mom_hbm.at[OWNERS * j + d], ps.at[j], ld_sem.at[j]).start()

    barrier = pltpu.get_barrier_semaphore()
    for k in range(1, OWNERS):
        pl.semaphore_signal(barrier, inc=1, device_id={"data": (d + k) % 4}, device_id_type=MESH)
    pl.semaphore_wait(barrier, OWNERS - 1)

    pos_copy.wait()

    def fill_theta(m, _):
        th[pl.ds(pl.multiple_of(m * LANES, LANES), LANES), :] = gbuf[m].astype(BF16)
        return 0

    lax.fori_loop(0, OWNERS * blocks, fill_theta, 0)
    for j in range(blocks):
        ts[j] = gbuf[OWNERS * j + d]
        pltpu.make_async_copy(mom_hbm.at[OWNERS * j + d], ps.at[j], ld_sem.at[j]).wait()
    hsum[...] = jnp.zeros_like(hsum)
    lacc[...] = jnp.zeros_like(lacc)

    def residual(n0, width, zt):
        half = y_ref[:, pl.ds(n0, width)]
        rt[:, pl.ds(n0, width)] = (half - 0.5 * jnp.tanh(0.5 * zt)).astype(BF16)

    def loss_rows(i):
        acc, prod = None, None
        for k in range(nb // LANES):
            n0 = pl.multiple_of(i * nb + k * LANES, LANES)
            zt = zs[pl.ds(n0, LANES), :]
            zs[pl.ds(n0, LANES), :] = jnp.zeros((LANES, LANES), F32)
            mag = jnp.abs(zt)
            line = 0.5 * mag - y_ref[:, pl.ds(n0, LANES)] * zt
            soft = 1.0 + jnp.exp(-mag)
            acc, prod = (line, soft) if acc is None else (acc + line, prod * soft)
        lacc[...] += acc + jnp.log(prod)

    def loss_span(lo, hi):
        lax.fori_loop(lo, hi, lambda i, _: (loss_rows(i), 0)[1], 0)

    def fold_loss(t):
        lt = lacc[...].T
        hsum[t] += jnp.sum(lt.reshape(LANES // 8, 8, LANES), axis=0)
        lacc[...] = jnp.zeros_like(lacc)

    def a_copy(j):
        return rcopy(gbuf.at[pl.ds(OWNERS * j + 2 * (1 - core), 2)], ra.at[pl.ds(2 * j, 2)], a_send.at[j], a_recv.at[j], sib)

    def b_copy(j):
        return rcopy(gbuf.at[OWNERS * j + 2 * core + 1 - xi], rb.at[j], b_send.at[j], b_recv.at[j], par)

    def th_rows(j, owner):
        return th.at[pl.ds(pl.multiple_of((OWNERS * j + owner) * LANES, LANES), LANES)]

    def ts_copy(j):
        return rcopy(th_rows(j, d), th_rows(j, d), ts_send.at[j], ts_recv.at[j], sib)

    def tx_copy(j):
        return rcopy(th_rows(j, d), th_rows(j, d), tx_send.at[j], tx_recv.at[j], par)

    def tf_copy(j):
        return rcopy(th_rows(j, par), th_rows(j, par), tf_send.at[j], tf_recv.at[j], sib)

    def own_copies(src, out, j, local, s_s, s_r, x_s, x_r):
        row = OWNERS * j + d
        return (
            lambda: pltpu.make_async_copy(src.at[j], out.at[row], local.at[j]),
            lambda: rcopy(src.at[j], out.at[row], x_s.at[j], x_r.at[j], par),
            lambda: rcopy(src.at[j], out.at[row], s_s.at[j], s_r.at[j], sib),
        )

    def pos_copies(j):
        return own_copies(ts, pos_out, j, ql_sem, qs_send, qs_recv, qx_send, qx_recv)

    def mom_copies(j):
        return own_copies(ps, mom_out, j, ol_sem, ts_send, ts_recv, tx_send, tx_recv)

    def pos_forward(j):
        row = OWNERS * j + par
        return rcopy(pos_out.at[row], pos_out.at[row], qf_send.at[j], qf_recv.at[j], sib)

    def mom_forward(j):
        row = OWNERS * j + par
        return rcopy(mom_out.at[row], mom_out.at[row], tf_send.at[j], tf_recv.at[j], sib)

    def stage1(j):
        a_copy(j).wait()
        away = OWNERS * j + 2 * core + 1 - xi
        gbuf[away] = gbuf[away] + ra[2 * j + 1 - xi]
        b_copy(j).start()

    def stage2(j, t):
        b_copy(j).wait()
        mine = OWNERS * j + 2 * core + xi
        q = ts[j]
        g = (gbuf[mine] + ra[2 * j + xi] + rb[j]).T - q * (1.0 / PRIOR_VAR)
        p = ps[j] + (0.5 * eps_ref[pl.ds(t, 1), :]) * g
        e = 0.5 * (p * p) + (0.5 / PRIOR_VAR) * (q * q)
        hsum[t] += jnp.sum(e.reshape(LANES // 8, 8, LANES), axis=0)

        @pl.when(t < steps)
        def _():
            step = eps_ref[pl.ds(t + 1, 1), :]
            pn = p + (0.5 * step) * g
            qn = q + step * pn
            th[pl.ds(pl.multiple_of((OWNERS * j + d) * LANES, LANES), LANES), :] = qn.astype(BF16)
            tx_copy(j).start()
            ts_copy(j).start()
            ps[j] = pn
            ts[j] = qn

        @pl.when(t == steps)
        def _():
            ps[j] = p
            for c in mom_copies(j):
                c().start()

    def stage3(j):
        tx_copy(j).wait()
        tf_copy(j).start()

    def stage4(j):
        ts_copy(j).wait()
        tf_copy(j).wait()

    def grad_block(j):
        res = jnp.dot(rt[...], xv[:, j * fb:(j + 1) * fb], preferred_element_type=F32)
        for k in range(OWNERS):
            gbuf[OWNERS * j + 2 * (k % 2) + k // 2] = res[:, k * LANES:(k + 1) * LANES]
        a_copy(j).start()

    def grad_phase(t):
        grad_block(0)
        grad_block(1)
        stage1(0)
        grad_block(2)
        stage1(1)
        grad_block(3)
        stage1(2)
        grad_block(4)
        stage2(0, t)
        stage1(3)
        grad_block(5)
        stage2(1, t)
        stage1(4)

    def logit_pieces(c0, h):
        cols = pl.ds(c0, fb)
        if h == 0:
            tt[...] = th[cols, :].T
        n0 = h * (rows // 2)
        for flat, size in PIECES:
            x = xv[n0:n0 + size, cols]
            if flat:
                yield n0, size, flat, jnp.dot(x, th[cols, :], preferred_element_type=F32)
            else:
                yield n0, size, flat, lax.dot_general(tt[...], x, (((1,), (1,)), ((), ())), preferred_element_type=F32)
            n0 += size

    def chunk_load(k):
        return pltpu.make_async_copy(turned.at[k], xt, c_sem)

    def turned_block(j, k):
        h = TURNED[k][1]
        if h == 0:
            tt[...] = th[pl.ds(pl.multiple_of(j * fb, fb), fb), :].T
        chunk_load(k).wait()
        flats = []
        for flat, size in PIECES:
            flats += [flat] * (size // LANES)
        for i in range(rows // 2 // nb):
            z = jnp.dot(tt[...], xt[i], preferred_element_type=F32)
            for m in range(nb // LANES):
                n0 = i * nb + m * LANES
                tile = slice(h * (rows // 2) + n0, h * (rows // 2) + n0 + LANES)
                zt = z[:, m * LANES:(m + 1) * LANES]
                zs[tile, :] += zt.T if flats[n0 // LANES] else zt
        chunk_load((k + 1) % len(TURNED)).start()

    def turned_write(i, m):
        half = rows // 2 // nb
        slot = 2 * (i % 2) + m
        return pltpu.make_async_copy(xt.at[slot], turned.at[2 * m + i // half, i % half], w_sem.at[slot])

    def make_turned(i):
        for m in range(2):
            pl.when(i >= 2)(lambda m=m: turned_write(i - 2, m).wait())
            c0 = pl.multiple_of((3 * m + i // (rows // 2 // nb)) * fb, fb)
            xt[2 * (i % 2) + m] = xv[tiles_of(i * nb), pl.ds(c0, fb)].T
        for m in range(2):
            turned_write(i, m).start()

    def plain_block(j, h):
        for n0, size, flat, z in logit_pieces(pl.multiple_of(j * fb, fb), h):
            if flat:
                zs[n0:n0 + size, :] += z
            else:
                for k in range(0, size, LANES):
                    zs[n0 + k:n0 + k + LANES, :] += z[:, k:k + LANES]

    def logit_block(j, h):
        mine = [k for k in range(len(TURNED)) if TURNED[k][1] == h]
        hit = j == TURNED[mine[0]][0]
        for k in mine[1:]:
            hit = jnp.logical_or(hit, j == TURNED[k][0])
        for k in mine:
            pl.when(j == TURNED[k][0])(functools.partial(turned_block, j, k))
        pl.when(jnp.logical_not(hit))(functools.partial(plain_block, j, h))

    def tiles_of(n0):
        return pl.ds(pl.multiple_of(n0, nb), nb)

    def finish_rows(i, z):
        for k in range(nb // LANES):
            zt = z[k * LANES:(k + 1) * LANES].T
            n0 = i * nb + k * LANES
            if not isinstance(n0, int):
                n0 = pl.multiple_of(n0, LANES)
            zs[pl.ds(n0, LANES), :] = zt
            residual(n0, LANES, zt)

    def last_block(j, h):
        for n0, size, flat, z in logit_pieces(j * fb, h):
            for k in range(0, size, LANES):
                tile = slice(n0 + k, n0 + k + LANES)
                zt = (zs[tile, :] + z[k:k + LANES]).T if flat else zs[tile, :] + z[:, k:k + LANES]
                zs[tile, :] = zt
                residual(n0 + k, LANES, zt)

    def logit_phase(t):
        stage3(0)

        def body(j, _):
            @pl.when(j == 1)
            def _():
                stage2(3, t)

            @pl.when((j == 3) & (t == steps - 1))
            def _():
                for k in range(blocks):
                    for c in pos_copies(k):
                        c().start()

            stage4(j)
            logit_block(j, 0)

            @pl.when(j == 1)
            def _():
                stage2(4, t)

            @pl.when(j == 2)
            def _():
                stage2(5, t)

            stage3(j + 1)
            logit_block(j, 1)
            return 0

        lax.fori_loop(0, blocks - 1, body, 0)
        stage4(blocks - 1)
        last_block(blocks - 1, 0)
        last_block(blocks - 1, 1)

    def first_rows(i, _):
        x_copy(i).wait()
        make_turned(i)
        finish_rows(i, jnp.dot(xv[tiles_of(i * nb), :], th[...], preferred_element_type=F32))
        return 0

    lax.fori_loop(0, rows // nb, first_rows, 0)
    for i in range(rows // nb - 2, rows // nb):
        for m in range(2):
            turned_write(i, m).wait()
    chunk_load(0).start()

    def leap(t, _):
        grad_phase(t)
        loss_span(0, 5)
        stage2(2, t)
        stage1(5)
        loss_span(5, 8)
        fold_loss(t)

        @pl.when(t < steps)
        def _():
            logit_phase(t)

        return 0

    lax.fori_loop(0, steps + 1, leap, 0)

    chunk_load(0).wait()

    for j in range(3, blocks):
        stage2(j, steps)
    for j in range(blocks):
        for c in pos_copies(j)[:2]:
            c().wait()
        pos_forward(j).start()

    hall[d] = jnp.sum(hsum[...], axis=1)[1:]

    def h_copy(k):
        return rcopy(hall.at[d], hall.at[d], hs_send.at[k - 1], h_recv.at[k - 1], (d + k) % 4)

    for k in range(1, OWNERS):
        h_copy(k).start()
    for j in range(blocks):
        local, cross, side = mom_copies(j)
        cross().wait()
        mom_forward(j).start()
        local().wait()
        side().wait()
    for k in range(1, OWNERS):
        h_copy(k).wait()
    h_out[...] = hall[0] + hall[1] + hall[2] + hall[3]
    for j in range(blocks):
        pos_copies(j)[2]().wait()
        pos_forward(j).wait()
        mom_forward(j).wait()


def solution(mesh):
    row_spec = P("data", None)
    chain_spec = P(None, "parts")

    def local_chains(feat_rows, labels, pos_init, mom_init, step_sizes):
        rows, feats = feat_rows.shape
        steps, chains = step_sizes.shape
        tiles = feats // LANES
        blocks = tiles // OWNERS
        label_row = labels.astype(F32)[None, :] - 0.5
        eps = jnp.concatenate([jnp.zeros((1, chains), F32), step_sizes], axis=0)
        dma = pltpu.SemaphoreType.DMA
        turned_shape = (rows // 2048, OWNERS * LANES, 1024)
        any_space = pl.BlockSpec(memory_space=pl.ANY)
        vmem = pl.BlockSpec(memory_space=pltpu.VMEM)
        cube = jax.ShapeDtypeStruct((tiles, LANES, chains), F32)
        positions, momentum, energies, _ = pl.pallas_call(
            functools.partial(hmc_kernel, rows, feats, steps),
            out_shape=(
                cube, cube, jax.ShapeDtypeStruct((steps, chains), F32),
                jax.ShapeDtypeStruct((len(TURNED),) + turned_shape, BF16)),
            in_specs=[any_space, vmem, any_space, any_space, vmem],
            out_specs=(any_space, any_space, vmem, any_space),
            scratch_shapes=[
                pltpu.VMEM((rows, feats), BF16),
                pltpu.VMEM((rows, chains), F32),
                pltpu.VMEM((chains, rows), BF16),
                pltpu.VMEM((feats, chains), BF16),
                pltpu.VMEM((chains, OWNERS * LANES), BF16),
                pltpu.VMEM(turned_shape, BF16),
                pltpu.VMEM((tiles, LANES, chains), F32),
                pltpu.VMEM((2 * blocks, LANES, chains), F32),
                pltpu.VMEM((blocks, LANES, chains), F32),
                pltpu.VMEM((blocks, LANES, chains), F32),
                pltpu.VMEM((blocks, LANES, chains), F32),
                pltpu.VMEM((steps + 1, 8, chains), F32),
                pltpu.VMEM((OWNERS, steps, chains), F32),
                pltpu.VMEM((chains, LANES), F32),
                dma((rows // 1024,)),
                dma((blocks + 1,)),
                dma((rows // 2048,)),
                dma,
            ]
            + [dma((blocks,)) for _ in range(10)]
            + [dma((blocks,)) for _ in range(7)]
            + [dma((blocks,)), dma((OWNERS - 1,)), dma((OWNERS - 1,))],
            compiler_params=pltpu.CompilerParams(
                collective_id=0, has_side_effects=True, vmem_limit_bytes=67043328),
            name="hmc",
        )(feat_rows, label_row, pos_init.reshape(cube.shape), mom_init.reshape(cube.shape), eps)
        return positions.reshape(feats, chains), momentum.reshape(feats, chains), energies

    return jax.shard_map(
        local_chains, mesh=mesh,
        in_specs=(row_spec, P("data"), chain_spec, chain_spec, chain_spec),
        out_specs=(chain_spec, chain_spec, chain_spec), check_vma=False)
```
